32 devices in a mesh: paths: 4 (over y, core), contract: 8 (over z, x).
Axes of the slice: x: 2, y: 2, z: 4, core: 2. Of those that a mesh axis runs over, the one named last changes fastest.
Arguments:
- prices: float32 [1, 512], P(None, 'paths'), may hold values from -6 to 6
- terminal: bfloat16 [128, 512, 128], P('contract', 'paths'), may hold values from -6 to 6
- band: int32 [128], replicated, may hold values from 32 to 128
- position: int32 [128], replicated, may hold values from 0 to 127, as said below
- actions: int32 [128, 3], replicated, may hold values from -3 to 3
- degree: int32 [128], replicated, may hold values from 2 to 7
- volume: float32 [128], replicated, may hold values from 0.05 to 0.5
Outputs:
- valued: bfloat16 [128, 512, 128], P('contract', 'paths')
The draws below stay inside these ranges and needn't reach their ends.
Inputs may be any that keep to these rules, and one draw needn't show every extreme that they name: A permutation of the contracts; contract c goes to new block position[c] // 16. Each old block of 16 contracts sends exactly 2 contracts to each of the 8 new blocks.
All inputs are finite; a program needn't handle non-finite values.
Results may differ from the reference program's by a relative error of at most 0.0038.
Values may be sent and summed in bfloat16 or wider, within the bound.
No kernel may reach another device: no remote copies, remote signals or barrier semaphores. Data moves between devices by JAX's collectives and lax.ppermute only.
A program may use at most 64 MiB of HBM per device.

```python
import math
import jax
import jax.numpy as jnp
from jax import lax

CAP = 2
LEVELS = 128
SECTIONS = 1
BASIS = 8
ACTIONS = 3
MOVE = 3
CON_DEV = 16
BLOCKS = 8
CONTRACTS = 128
PATHS = 512


def draw_position(key, part):
    first_key, second_key, third_key = jax.random.split(jax.random.fold_in(key, 7301), 3)
    groups = CON_DEV // CAP
    offsets = jax.random.permutation(first_key, BLOCKS)[:groups]
    ranking = jax.vmap(lambda sub: jax.random.permutation(sub, CON_DEV))(jax.random.split(second_key, BLOCKS))
    shuffles = jax.vmap(lambda sub: jax.random.permutation(sub, CON_DEV))(jax.random.split(third_key, BLOCKS))
    source_block = jnp.arange(BLOCKS, dtype=jnp.int32)[:, None]
    target = (source_block + offsets[ranking // CAP]) % BLOCKS
    new_slot = shuffles[target, ranking]
    return (target * CON_DEV + new_slot).reshape(-1).astype(jnp.int32)


def set_ends(drawn, rng, low, top_value):
    spot = [jax.random.randint(jax.random.fold_in(rng, axis), (), 0, length) for axis, length in enumerate(drawn.shape)]
    widest = drawn.shape.index(max(drawn.shape))
    neighbour = spot[:widest] + [(spot[widest] + 1) % drawn.shape[widest]] + spot[widest + 1:]
    return drawn.at[tuple(spot)].set(low).at[tuple(neighbour)].set(top_value)


def block_levels(own_key, dims, cuts, least, high):
    loudness = 1.0
    for dim, parts in cuts:
        heights = jax.random.uniform(jax.random.fold_in(jax.random.fold_in(own_key, 6), dim), (parts,), jnp.float32, least / len(cuts), high / len(cuts))
        loudness = loudness * jnp.repeat(jnp.exp(heights), dims[dim] // parts).reshape((-1,) + (1,) * (len(dims) - 1 - dim))
    return loudness


def gaussian(stream_key, dims, scale, limit, cuts=(), held_as=jnp.bfloat16):
    drawn = jax.random.normal(stream_key, dims, jnp.float32) * scale
    if len(cuts) > 0:
        drawn = block_levels(stream_key, dims, cuts, -0.22, 0.18) * drawn
    return jnp.clip(drawn, min=-limit, max=limit).astype(held_as)


def setup_inputs(seed: int = 0) -> dict:
    arg_keys = jax.random.split(jax.random.key(seed), 8)
    prices = gaussian(arg_keys[0], (SECTIONS, PATHS), 1.0, 6.0, ((1, 4),), jnp.float32)
    terminal = gaussian(arg_keys[1], (CONTRACTS, PATHS, LEVELS), 1.0, 6.0, ((0, 8), (1, 4)))
    band = set_ends(jax.random.randint(arg_keys[2], (CONTRACTS,), LEVELS // 4, LEVELS + 1), jax.random.fold_in(arg_keys[2], 1), LEVELS // 4, LEVELS).astype(jnp.int32)
    position = draw_position(jax.random.fold_in(arg_keys[7], 71), 0)
    actions = set_ends(jax.random.randint(arg_keys[4], (CONTRACTS, ACTIONS), -MOVE, MOVE + 1), jax.random.fold_in(arg_keys[4], 1), -MOVE, MOVE).astype(jnp.int32)
    degree = set_ends(jax.random.randint(arg_keys[5], (CONTRACTS,), 2, BASIS), jax.random.fold_in(arg_keys[5], 1), 2, BASIS - 1).astype(jnp.int32)
    volume = jnp.clip(jnp.exp(jax.random.uniform(arg_keys[6], (CONTRACTS,), jnp.float32, math.log(0.05), math.log(0.5))), 0.05, 0.5)
    return {"prices": prices, "terminal": terminal, "band": band, "position": position, "actions": actions, "degree": degree, "volume": volume}


RIDGE = 0.05
DISCOUNT = 0.98
SPOT_SCALE = 0.25

def chebyshev(prices_row):
    scaled = jnp.tanh(prices_row)
    series = [jnp.ones_like(scaled), scaled]
    for order in range(2, BASIS):
        series.append(2.0 * scaled * series[-1] - series[-2])
    return jnp.stack(series[:BASIS])

def regress(gram, moments, path_count, degree_block):
    orders = jnp.arange(BASIS, dtype=jnp.int32)
    keep_basis = (orders[None, :] <= degree_block[:, None]).astype(jnp.float32)
    identity = jnp.eye(BASIS, dtype=jnp.float32)
    system = keep_basis[:, :, None] * keep_basis[:, None, :] * (gram / path_count)[None]
    system = system + (1.0 - keep_basis)[:, :, None] * identity[None] + RIDGE * identity[None]
    scaled_moments = keep_basis[:, :, None] * (moments / path_count)
    factor = jnp.linalg.cholesky(system)
    halfway = lax.linalg.triangular_solve(factor, scaled_moments, left_side=True, lower=True)
    return lax.linalg.triangular_solve(factor, halfway, left_side=True, lower=True, transpose_a=True)

def decide(values_now, estimate, spot_price, band_block, action_block, volume_block):
    levels = jnp.arange(LEVELS, dtype=jnp.int32)
    living = levels[None, :] < band_block[:, None]
    padded = jnp.pad(estimate, ((0, 0), (0, 0), (MOVE, MOVE)))
    optimum = DISCOUNT * estimate
    for offset in range(-MOVE, MOVE + 1):
        if offset == 0:
            continue
        allowed = jnp.any(action_block == offset, axis=1)
        target_level = levels + offset
        inside = (target_level[None, :] >= 0) & (target_level[None, :] < band_block[:, None])
        moved = padded[:, :, MOVE + offset:MOVE + offset + LEVELS]
        candidate = -offset * volume_block[:, None, None] * spot_price[None, :, None] + DISCOUNT * moved
        usable = allowed[:, None, None] & inside[:, None, :]
        optimum = jnp.where(usable, jnp.maximum(optimum, candidate), optimum)
    return jnp.where(living[:, None, :], optimum + DISCOUNT * (values_now - estimate), 0.0)

def reference(prices, terminal, band, position, actions, degree, volume):
    highest = lax.Precision.HIGHEST
    basis_all = jnp.stack([chebyshev(prices[section]) for section in range(SECTIONS)])
    grams = jnp.einsum('skp,sjp->skj', basis_all, basis_all, precision=highest)
    spots = jnp.exp(SPOT_SCALE * prices)
    arrival = jnp.argsort(position).astype(jnp.int32).reshape(CONTRACTS // CON_DEV, CON_DEV)

    def value_block(contract_ids):
        values_now = terminal[contract_ids].astype(jnp.float32)
        band_block = band[contract_ids]
        action_block = actions[contract_ids]
        degree_block = degree[contract_ids]
        volume_block = volume[contract_ids]
        for section in range(SECTIONS - 1, -1, -1):
            moments = jnp.einsum('kp,cpl->ckl', basis_all[section], values_now, precision=highest)
            fitted = regress(grams[section], moments, PATHS, degree_block)
            estimate = jnp.einsum('kp,ckl->cpl', basis_all[section], fitted, precision=highest)
            values_now = decide(values_now, estimate, spots[section], band_block, action_block, volume_block)
        return values_now.astype(jnp.bfloat16)
    return lax.map(value_block, arrival).reshape(CONTRACTS, PATHS, LEVELS)
```

```python
import functools

import jax
import jax.numpy as jnp
from jax import lax
from jax.experimental import pallas as pl
from jax.experimental.pallas import tpu as pltpu
from jax.sharding import PartitionSpec as P

BASIS = 8
RIDGE = 0.05
DISCOUNT = 0.98
SPOT_SCALE = 0.25
FAR = -1e30
HIGHEST = lax.Precision.HIGHEST
BF16 = jnp.bfloat16
F32 = jnp.float32

VMEM = pl.BlockSpec(memory_space=pltpu.VMEM)
SMEM = pl.BlockSpec(memory_space=pltpu.SMEM)


def peer_of(index, step, count):
    if count & (count - 1) == 0:
        return index ^ step
    return (index + step) % count


def source_of(index, step, count):
    if count & (count - 1) == 0:
        return index ^ step
    return (index + count - step) % count


def exchange(x, axis, step, count):
    pairs = [(i, peer_of(i, step, count)) for i in range(count)]
    return lax.ppermute(x, axis, pairs)


def group_kernel(blocks, con, cap, position_ref, terminal_ref, *refs):
    outs, (counts, sources) = refs[:blocks], refs[blocks:]
    me = lax.axis_index("contract")

    def clear(b, carry):
        counts[b] = 0
        return carry

    lax.fori_loop(0, blocks, clear, 0, unroll=True)

    def place(i, carry):
        target = position_ref[me * con + i] // con
        rank = counts[target]
        counts[target] = rank + 1
        sources[target * cap + rank] = i
        return carry

    lax.fori_loop(0, con, place, 0, unroll=True)
    for k in range(blocks):
        peer = peer_of(me, k, blocks)
        for j in range(cap):
            outs[k][j] = terminal_ref[sources[peer * cap + j]]


def chebyshev(prices):
    scaled = jnp.tanh(prices)
    series = [jnp.ones_like(scaled), scaled]
    for _ in range(2, BASIS):
        series.append(2.0 * scaled * series[-1] - series[-2])
    return jnp.concatenate(series, axis=0)


def split(x):
    high = x.astype(BF16).astype(F32)
    return high, x - high


def basis_kernel(prices_ref, rows_ref, columns_ref, gram_ref):
    prices = prices_ref[...]
    basis = chebyshev(prices)
    high, low = split(basis)
    rows_ref[...] = jnp.concatenate([high, low], axis=0).astype(BF16)
    spot = jnp.exp(SPOT_SCALE * prices)
    spot_high, spot_low = split(spot)
    extra = jnp.concatenate(
        [spot_high, spot_low, spot_high, jnp.ones_like(spot), jnp.zeros((4, spot.shape[1]), F32)],
        axis=0,
    )
    stacked = jnp.concatenate([high, low, high, extra], axis=0)
    columns_ref[...] = stacked.T.astype(BF16)
    gram = lax.dot_general(
        basis, basis, (((1,), (1,)), ((), ())), precision=HIGHEST, preferred_element_type=F32
    )
    gram = jnp.concatenate([gram, jnp.zeros((BASIS, 128 - BASIS), F32)], axis=1)
    gram_high, gram_low = split(gram)
    gram_ref[...] = jnp.concatenate([gram_high, gram_low], axis=0).astype(BF16)


def moment_kernel(blocks, cap, rows_ref, gram_ref, *refs):
    values, out_ref = refs[:blocks], refs[blocks]
    rows = rows_ref[...]
    count = blocks * cap
    for k in range(blocks):
        pieces = []
        for j in range(cap):
            both = jnp.dot(rows, values[k][j], preferred_element_type=F32)
            pieces.append(both[:BASIS] + both[BASIS:])
        out_ref[pl.ds(k * cap * BASIS, cap * BASIS)] = jnp.concatenate(pieces, axis=0).astype(BF16)
    out_ref[pl.ds(count * BASIS, 2 * BASIS)] = gram_ref[...]


def inverse_factor(system):
    row = lax.broadcasted_iota(jnp.int32, (BASIS, 128), 0)
    lane = lax.broadcasted_iota(jnp.int32, (BASIS, 128), 1)
    picks = jnp.concatenate([jnp.where(lane == i, system, 0.0) for i in range(BASIS)], axis=0)
    spread = jnp.dot(picks, jnp.ones((128, 128), F32), precision=HIGHEST, preferred_element_type=F32)
    left = [spread[i * BASIS : (i + 1) * BASIS] for i in range(BASIS)]
    right = [jnp.where(row == i, 1.0, 0.0) for i in range(BASIS)]
    pivots = jnp.ones((BASIS, 128), F32)
    for k in range(BASIS):
        pivot = jnp.broadcast_to(left[k][k : k + 1], (BASIS, 128))
        recip = 1.0 / pivot
        pivots = jnp.where(row == k, recip, pivots)
        factor = jnp.where(row > k, left[k] * recip, 0.0)
        for i in range(k + 1, BASIS):
            left[i] = left[i] - factor * jnp.broadcast_to(left[i][k : k + 1], (BASIS, 128))
        for i in range(k + 1):
            right[i] = right[i] - factor * jnp.broadcast_to(right[i][k : k + 1], (BASIS, 128))
    matrix = jnp.zeros((BASIS, 128), F32)
    for i in range(BASIS):
        matrix = jnp.where(lane == i, right[i], matrix)
    return matrix[:, :BASIS], pivots


def decide_kernel(blocks, cap, shards, acts, path_count, meta_ref, volume_ref, columns_ref, *refs):
    values = refs[:blocks]
    parts = refs[blocks : blocks + shards]
    out_ref = refs[blocks + shards]
    me = lax.axis_index("contract")
    count = blocks * cap
    total = parts[0][...].astype(F32)
    for part in parts[1:]:
        total = total + part[...].astype(F32)
    row = lax.broadcasted_iota(jnp.int32, (BASIS, 128), 0)
    lane = lax.broadcasted_iota(jnp.int32, (BASIS, 128), 1)
    gram = total[count * BASIS : (count + 1) * BASIS] + total[(count + 1) * BASIS :]
    system = gram * (1.0 / path_count) + jnp.where(row == lane, RIDGE, 0.0)
    lower, pivots = inverse_factor(system)
    moments = jnp.concatenate([total[a * BASIS : (a + 1) * BASIS] for a in range(count)], axis=1)
    solved = jnp.dot(lower, moments, precision=HIGHEST, preferred_element_type=F32)
    scale = pivots * (DISCOUNT / path_count)
    slots = [source_of(me, k, blocks) * cap + j for k in range(blocks) for j in range(cap)]
    width = 3 + acts
    kept = []
    for a in range(count):
        degree = meta_ref[slots[a] * width + 2]
        kept.append(jnp.where(row <= degree, solved[:, a * 128 : (a + 1) * 128] * scale, 0.0))
    fitted_all = lax.dot_general(
        lower,
        jnp.concatenate(kept, axis=1),
        (((0,), (0,)), ((), ())),
        precision=HIGHEST,
        preferred_element_type=F32,
    )
    columns = columns_ref[...]
    level = lax.broadcasted_iota(jnp.int32, (1, 128), 1)
    for k in range(blocks):
        for j in range(cap):
            a = k * cap + j
            base = slots[a] * width
            place, band = meta_ref[base], meta_ref[base + 1]
            volume = volume_ref[slots[a]]
            fitted = fitted_all[:, a * 128 : (a + 1) * 128]
            tables = []
            for act in range(acts + 1):
                if act == 0:
                    moved = fitted
                    extra = jnp.zeros((BASIS, 128), F32)
                else:
                    offset = meta_ref[base + 2 + act]
                    shift = jnp.where(offset > 0, 128 - offset, -offset)
                    moved = pltpu.roll(fitted, shift, 1)
                    price = jnp.full((BASIS, 128), -offset.astype(F32) * volume, F32)
                    price_high, price_low = split(price)
                    target = lane + offset
                    usable = (target >= 0) & (target < band)
                    blocked = jnp.where(usable, 0.0, FAR)
                    extra = jnp.where(row < 2, price_high, jnp.where(row == 2, price_low, 0.0))
                    extra = jnp.where(row == 3, blocked, extra)
                moved_high, moved_low = split(moved)
                tables.append(
                    jnp.concatenate([moved_high, moved_high, moved_low, extra], axis=0).astype(BF16)
                )
            table = jnp.concatenate(tables, axis=1)
            estimates = jnp.dot(columns, table, preferred_element_type=F32)
            stay = estimates[:, :128]
            optimum = stay
            for act in range(1, acts + 1):
                optimum = jnp.maximum(optimum, estimates[:, act * 128 : (act + 1) * 128])
            result = (optimum - stay) + DISCOUNT * values[k][j].astype(F32)
            out_ref[place] = jnp.where(level < band, result, 0.0).astype(BF16)


def arrivals(position, me, blocks, con, cap):
    target = (position // con).reshape(blocks, con)
    mine = target == me
    slot = jnp.arange(con, dtype=jnp.int32)
    earlier = slot[None, :, None] > slot[None, None, :]
    rank = jnp.sum(earlier & mine[:, None, :], axis=2)
    chosen = mine[:, None, :] & (rank[:, None, :] == jnp.arange(cap, dtype=jnp.int32)[None, :, None])
    first = jnp.arange(blocks, dtype=jnp.int32)[:, None] * con
    ids = jnp.sum(jnp.where(chosen, slot[None, None, :], 0), axis=2) + first
    return ids.reshape(-1)


def per_device(prices, terminal, band, position, actions, degree, volume):
    blocks = lax.axis_size("contract")
    shards = lax.axis_size("paths")
    me = lax.axis_index("contract")
    con, paths, levels = terminal.shape
    cap = con // blocks
    acts = actions.shape[1]
    path_count = paths * shards
    piece = jax.ShapeDtypeStruct((cap, paths, levels), BF16)
    groups = pl.pallas_call(
        functools.partial(group_kernel, blocks, con, cap),
        out_shape=[piece] * blocks,
        in_specs=[SMEM, VMEM],
        out_specs=[VMEM] * blocks,
        scratch_shapes=[pltpu.SMEM((blocks,), jnp.int32), pltpu.SMEM((con,), jnp.int32)],
        name="group",
    )(position, terminal)
    values = [groups[0]] + [exchange(groups[k], "contract", k, blocks) for k in range(1, blocks)]
    ids = arrivals(position, me, blocks, con, cap)
    table = jnp.concatenate(
        [position[:, None] - me * con, band[:, None], degree[:, None], actions], axis=1
    )
    match = ids[:, None] == jnp.arange(position.shape[0], dtype=jnp.int32)[None, :]
    meta = jnp.sum(jnp.where(match[:, :, None], table[None], 0), axis=1).reshape(-1)
    volumes = jnp.sum(jnp.where(match, volume[None, :], 0.0), axis=1)
    rows, columns, gram = pl.pallas_call(
        basis_kernel,
        out_shape=[
            jax.ShapeDtypeStruct((2 * BASIS, paths), BF16),
            jax.ShapeDtypeStruct((paths, 4 * BASIS), BF16),
            jax.ShapeDtypeStruct((2 * BASIS, 128), BF16),
        ],
        in_specs=[VMEM],
        out_specs=[VMEM] * 3,
        name="basis",
    )(prices)
    moments = pl.pallas_call(
        functools.partial(moment_kernel, blocks, cap),
        out_shape=jax.ShapeDtypeStruct(((con + 2) * BASIS, levels), BF16),
        in_specs=[VMEM] * (2 + blocks),
        out_specs=VMEM,
        name="moments",
    )(rows, gram, *values)
    parts = [moments] + [exchange(moments, "paths", k, shards) for k in range(1, shards)]
    return pl.pallas_call(
        functools.partial(decide_kernel, blocks, cap, shards, acts, path_count),
        out_shape=jax.ShapeDtypeStruct((con, paths, levels), BF16),
        in_specs=[SMEM, SMEM] + [VMEM] * (1 + blocks + shards),
        out_specs=VMEM,
        name="decide",
    )(meta, volumes, columns, *values, *parts)


def solution(mesh):
    in_specs = (P(None, "paths"), P("contract", "paths", None), P(), P(), P(), P(), P())
    out_specs = P("contract", "paths", None)
    return jax.shard_map(
        per_device, mesh=mesh, in_specs=in_specs, out_specs=out_specs, check_vma=False
    )
```

```python
import functools

import jax
import jax.numpy as jnp
from jax import lax
from jax.experimental import pallas as pl
from jax.experimental.pallas import tpu as pltpu
from jax.sharding import PartitionSpec as P

BASIS = 8
RIDGE = 0.05
DISCOUNT = 0.98
SPOT_SCALE = 0.25
FAR = -1e30
HIGHEST = lax.Precision.HIGHEST
BF16 = jnp.bfloat16
F32 = jnp.float32

VMEM = pl.BlockSpec(memory_space=pltpu.VMEM)
SMEM = pl.BlockSpec(memory_space=pltpu.SMEM)
HBM = pl.BlockSpec(memory_space=pltpu.MemorySpace.HBM)
DMA = pltpu.SemaphoreType.DMA

PARAMS = pltpu.CompilerParams(vmem_limit_bytes=16 * 1024 * 1024)


def peer_of(index, step, count):
    if count & (count - 1) == 0:
        return index ^ step
    return (index + step) % count


def source_of(index, step, count):
    if count & (count - 1) == 0:
        return index ^ step
    return (index + count - step) % count


def exchange(x, axis, step, count):
    pairs = [(i, peer_of(i, step, count)) for i in range(count)]
    return lax.ppermute(x, axis, pairs)


def group_kernel(blocks, con, cap, position_ref, terminal_ref, *refs):
    outs, (old, place, counts, sources, sems) = refs[:blocks], refs[blocks:]
    me = lax.axis_index("contract")
    load = pltpu.make_async_copy(terminal_ref, old, sems.at[0])
    load.start()
    places = pltpu.make_async_copy(position_ref, place, sems.at[1])
    places.start()

    def clear(b, carry):
        counts[b] = 0
        return carry

    lax.fori_loop(0, blocks, clear, 0, unroll=True)
    places.wait()

    def assign(i, carry):
        target = place[me * con + i] // con
        rank = counts[target]
        counts[target] = rank + 1
        sources[target * cap + rank] = i
        return carry

    lax.fori_loop(0, con, assign, 0, unroll=True)
    load.wait()
    for k in range(blocks):
        peer = peer_of(me, k, blocks)
        for j in range(cap):
            outs[k][j] = old[sources[peer * cap + j]]


def chebyshev(prices):
    scaled = jnp.tanh(prices)
    series = [jnp.ones_like(scaled), scaled]
    for _ in range(2, BASIS):
        series.append(2.0 * scaled * series[-1] - series[-2])
    return jnp.concatenate(series, axis=0)


def split(x):
    high = x.astype(BF16).astype(F32)
    return high, x - high


def prepare_kernel(blocks, con, cap, acts, *refs):
    tables, refs = refs[:6], refs[6:]
    (rows_ref, columns_ref, gram_ref, extra_ref, meta_ref), refs = refs[:5], refs[5:]
    local, (counts, ids, sems) = refs[:6], refs[6:]
    copies = [pltpu.make_async_copy(t, l, sems.at[i]) for i, (t, l) in enumerate(zip(tables, local))]
    for copy in copies:
        copy.start()
    for copy in copies:
        copy.wait()
    prices_ref, position_ref, band_ref, degree_ref, actions_ref, volume_ref = local
    me = lax.axis_index("contract")

    def scan(c, carry):
        block = c // con
        place = position_ref[c] - me * con
        here = (place >= 0) & (place < con)
        rank = jnp.where(c == block * con, 0, counts[0])
        counts[0] = jnp.where(here, rank + 1, rank)

        @pl.when(here)
        def _():
            ids[block * cap + rank] = c

        return carry

    lax.fori_loop(0, blocks * con, scan, 0, unroll=8)
    prices = prices_ref[...]
    basis = chebyshev(prices)
    high, low = split(basis)
    rows_ref[...] = jnp.concatenate([high, low], axis=0).astype(BF16)
    spot = jnp.exp(SPOT_SCALE * prices)
    spot_high, spot_low = split(spot)
    more = jnp.concatenate(
        [spot_high, spot_low, spot_high, jnp.ones_like(spot), jnp.zeros((4, spot.shape[1]), F32)],
        axis=0,
    )
    stacked = jnp.concatenate([high, low, high, more], axis=0)
    columns_ref[...] = stacked.T.astype(BF16)
    gram = lax.dot_general(
        basis, basis, (((1,), (1,)), ((), ())), precision=HIGHEST, preferred_element_type=F32
    )
    gram = jnp.concatenate([gram, jnp.zeros((BASIS, 128 - BASIS), F32)], axis=1)
    gram_high, gram_low = split(gram)
    gram_ref[...] = jnp.concatenate([gram_high, gram_low], axis=0).astype(BF16)
    row = lax.broadcasted_iota(jnp.int32, (BASIS, 128), 0)
    lane = lax.broadcasted_iota(jnp.int32, (BASIS, 128), 1)
    width = 3 + acts
    for k in range(blocks):
        source = source_of(me, k, blocks)
        for j in range(cap):
            a = k * cap + j
            c = ids[source * cap + j]
            band, volume = band_ref[c], volume_ref[c]
            meta_ref[a * width] = position_ref[c] - me * con
            meta_ref[a * width + 1] = band
            meta_ref[a * width + 2] = degree_ref[c]
            for act in range(acts):
                offset = actions_ref[act, c]
                meta_ref[a * width + 3 + act] = jnp.where(offset > 0, 128 - offset, -offset)
                price = jnp.full((BASIS, 128), -offset.astype(F32) * volume, F32)
                price_high, price_low = split(price)
                target = lane + offset
                usable = (target >= 0) & (target < band)
                extra = jnp.where(row < 2, price_high, jnp.where(row == 2, price_low, 0.0))
                extra_ref[a * acts + act] = jnp.where(
                    row == 3, jnp.where(usable, 0.0, FAR), extra
                )


def moment_kernel(blocks, cap, rows_ref, gram_ref, *refs):
    values, out_ref = refs[:blocks], refs[blocks]
    rows = rows_ref[...]
    count = blocks * cap
    for k in range(blocks):
        pieces = []
        for j in range(cap):
            both = jnp.dot(rows, values[k][j], preferred_element_type=F32)
            pieces.append(both[:BASIS] + both[BASIS:])
        out_ref[pl.ds(k * cap * BASIS, cap * BASIS)] = jnp.concatenate(pieces, axis=0).astype(BF16)
    out_ref[pl.ds(count * BASIS, 2 * BASIS)] = gram_ref[...]


def inverse_factor(system):
    row = lax.broadcasted_iota(jnp.int32, (BASIS, 128), 0)
    lane = lax.broadcasted_iota(jnp.int32, (BASIS, 128), 1)
    picks = jnp.concatenate([jnp.where(lane == i, system, 0.0) for i in range(BASIS)], axis=0)
    spread = jnp.dot(picks, jnp.ones((128, 128), F32), precision=HIGHEST, preferred_element_type=F32)
    left = [spread[i * BASIS : (i + 1) * BASIS] for i in range(BASIS)]
    right = [jnp.where(row == i, 1.0, 0.0) for i in range(BASIS)]
    pivots = jnp.ones((BASIS, 128), F32)
    for k in range(BASIS):
        pivot = jnp.broadcast_to(left[k][k : k + 1], (BASIS, 128))
        recip = 1.0 / pivot
        pivots = jnp.where(row == k, recip, pivots)
        factor = jnp.where(row > k, left[k] * recip, 0.0)
        for i in range(k + 1, BASIS):
            left[i] = left[i] - factor * jnp.broadcast_to(left[i][k : k + 1], (BASIS, 128))
        for i in range(k + 1):
            right[i] = right[i] - factor * jnp.broadcast_to(right[i][k : k + 1], (BASIS, 128))
    matrix = jnp.zeros((BASIS, 128), F32)
    for i in range(BASIS):
        matrix = jnp.where(lane == i, right[i], matrix)
    return matrix[:, :BASIS], pivots


def decide_kernel(blocks, cap, shards, acts, path_count, meta_ref, columns_ref, extra_ref, *refs):
    values, refs = refs[:blocks], refs[blocks:]
    parts, (out_ref, kept_out, sems) = refs[:shards], refs[shards:]
    count = blocks * cap
    total = parts[0][...].astype(F32)
    for part in parts[1:]:
        total = total + part[...].astype(F32)
    row = lax.broadcasted_iota(jnp.int32, (BASIS, 128), 0)
    lane = lax.broadcasted_iota(jnp.int32, (BASIS, 128), 1)
    gram = total[count * BASIS : (count + 1) * BASIS] + total[(count + 1) * BASIS :]
    system = gram * (1.0 / path_count) + jnp.where(row == lane, RIDGE, 0.0)
    lower, pivots = inverse_factor(system)
    moments = jnp.concatenate([total[a * BASIS : (a + 1) * BASIS] for a in range(count)], axis=1)
    solved = jnp.dot(lower, moments, precision=HIGHEST, preferred_element_type=F32)
    scale = pivots * (DISCOUNT / path_count)
    width = 3 + acts
    kept = []
    for a in range(count):
        degree = meta_ref[a * width + 2]
        kept.append(jnp.where(row <= degree, solved[:, a * 128 : (a + 1) * 128] * scale, 0.0))
    fitted_all = lax.dot_general(
        lower,
        jnp.concatenate(kept, axis=1),
        (((0,), (0,)), ((), ())),
        precision=HIGHEST,
        preferred_element_type=F32,
    )
    columns = columns_ref[...]
    level = lax.broadcasted_iota(jnp.int32, (1, 128), 1)
    copies = []
    for a in range(count):
        base = a * width
        place, band = meta_ref[base], meta_ref[base + 1]
        fitted = fitted_all[:, a * 128 : (a + 1) * 128]
        tables = []
        for act in range(acts + 1):
            if act == 0:
                moved = fitted
                extra = jnp.zeros((BASIS, 128), F32)
            else:
                moved = pltpu.roll(fitted, meta_ref[base + 2 + act], 1)
                extra = extra_ref[a * acts + act - 1]
            moved_high, moved_low = split(moved)
            tables.append(
                jnp.concatenate([moved_high, moved_high, moved_low, extra], axis=0).astype(BF16)
            )
        table = jnp.concatenate(tables, axis=1)
        estimates = jnp.dot(columns, table, preferred_element_type=F32)
        stay = estimates[:, :128]
        optimum = stay
        for act in range(1, acts + 1):
            optimum = jnp.maximum(optimum, estimates[:, act * 128 : (act + 1) * 128])
        result = (optimum - stay) + DISCOUNT * values[a // cap][a % cap].astype(F32)
        kept_out[a] = jnp.where(level < band, result, 0.0).astype(BF16)
        copy = pltpu.make_async_copy(kept_out.at[a], out_ref.at[place], sems.at[a])
        copy.start()
        copies.append(copy)
    for copy in copies:
        copy.wait()


def per_device(prices, terminal, band, position, actions, degree, volume):
    blocks = lax.axis_size("contract")
    shards = lax.axis_size("paths")
    con, paths, levels = terminal.shape
    cap = con // blocks
    acts = actions.shape[1]
    path_count = paths * shards
    count = con
    contracts = position.shape[0]
    piece = jax.ShapeDtypeStruct((cap, paths, levels), BF16)
    groups = pl.pallas_call(
        functools.partial(group_kernel, blocks, con, cap),
        out_shape=[piece] * blocks,
        in_specs=[HBM, HBM],
        out_specs=[VMEM] * blocks,
        scratch_shapes=[
            pltpu.VMEM((con, paths, levels), BF16),
            pltpu.SMEM((contracts,), jnp.int32),
            pltpu.SMEM((blocks,), jnp.int32),
            pltpu.SMEM((con,), jnp.int32),
            DMA((2,)),
        ],
        compiler_params=PARAMS,
        name="group",
    )(
        pltpu.with_memory_space_constraint(position, pltpu.MemorySpace.HBM),
        pltpu.with_memory_space_constraint(terminal, pltpu.MemorySpace.HBM),
    )
    moved = {}
    for k in range(1, blocks):
        moved[k] = exchange(groups[k], "contract", k, blocks)
    values = [groups[0]] + [moved[k] for k in range(1, blocks)]
    rows, columns, gram, extra, meta = pl.pallas_call(
        functools.partial(prepare_kernel, blocks, con, cap, acts),
        out_shape=[
            jax.ShapeDtypeStruct((2 * BASIS, paths), BF16),
            jax.ShapeDtypeStruct((paths, 4 * BASIS), BF16),
            jax.ShapeDtypeStruct((2 * BASIS, 128), BF16),
            jax.ShapeDtypeStruct((count * acts, BASIS, 128), F32),
            jax.ShapeDtypeStruct((count * (3 + acts),), jnp.int32),
        ],
        in_specs=[HBM] * 6,
        out_specs=[VMEM] * 4 + [SMEM],
        scratch_shapes=[
            pltpu.VMEM(prices.shape, F32),
            pltpu.SMEM((contracts,), jnp.int32),
            pltpu.SMEM((contracts,), jnp.int32),
            pltpu.SMEM((contracts,), jnp.int32),
            pltpu.SMEM((acts, contracts), jnp.int32),
            pltpu.SMEM((contracts,), F32),
            pltpu.SMEM((1,), jnp.int32),
            pltpu.SMEM((count,), jnp.int32),
            DMA((6,)),
        ],
        compiler_params=PARAMS,
        name="prepare",
    )(prices, position, band, degree, actions.T, volume)
    moments = pl.pallas_call(
        functools.partial(moment_kernel, blocks, cap),
        out_shape=jax.ShapeDtypeStruct(((count + 2) * BASIS, levels), BF16),
        in_specs=[VMEM] * (2 + blocks),
        out_specs=VMEM,
        compiler_params=PARAMS,
        name="moments",
    )(rows, gram, *values)
    parts = [moments] + [exchange(moments, "paths", k, shards) for k in range(1, shards)]
    return pl.pallas_call(
        functools.partial(decide_kernel, blocks, cap, shards, acts, path_count),
        out_shape=jax.ShapeDtypeStruct((con, paths, levels), BF16),
        in_specs=[SMEM] + [VMEM] * (2 + blocks + shards),
        out_specs=HBM,
        scratch_shapes=[pltpu.VMEM((count, paths, levels), BF16), DMA((count,))],
        compiler_params=PARAMS,
        name="decide",
    )(meta, columns, extra, *values, *parts)


def solution(mesh):
    in_specs = (P(None, "paths"), P("contract", "paths", None), P(), P(), P(), P(), P())
    out_specs = P("contract", "paths", None)
    return jax.shard_map(
        per_device, mesh=mesh, in_specs=in_specs, out_specs=out_specs, check_vma=False
    )
```
